32 devices in a mesh: dp: 8 (over y, x, core), mp: 4 (over z).
Axes of the slice: x: 2, y: 2, z: 4, core: 2. Of those that a mesh axis runs over, the one named last changes fastest.
Arguments:
- saved_query: bfloat16 [2048, 4096], P('dp', 'mp'), may hold values from -80 to 80
- saved_key: bfloat16 [2048, 1024], P('dp', 'mp'), may hold values from -16 to 16
- saved_value: bfloat16 [2048, 1024], P('dp', 'mp'), may hold values from -6 to 6
- grad_output: bfloat16 [2048, 4096], P('dp', 'mp'), may hold values from -24 to 24
- unit_server: int32 [64], P('dp'), may hold values from 0 to 7, as said below
- unit_place: int32 [64], P('dp'), may hold values from 0 to 7, as said below
- doc_length: int32 [8], P('dp'), may hold values from 1 to 256
- query_weight: bfloat16 [4096, 4096], P(None, 'mp'), may hold values from -0.078125 to 0.078125
- key_weight: bfloat16 [4096, 1024], P(None, 'mp'), may hold values from -0.078125 to 0.078125
- value_weight: bfloat16 [4096, 1024], P(None, 'mp'), may hold values from -0.078125 to 0.078125
Outputs:
- grad_input: float32 [2048, 4096], P('dp', 'mp')
The draws below stay inside these ranges and needn't reach their ends.
Inputs may be any that keep to these rules, and one draw needn't show every extreme that they name: `unit_server`: each server receives exactly 8 units, exactly one from the units of each device along dp; the units of one document block come from 8 different devices. The pairs (unit_server, unit_place) are all different, so each server's places 0 to 7 are each taken once.
All inputs are finite; a program needn't handle non-finite values.
Results may differ from the reference program's by a relative error of at most 0.011.
Values may be sent and summed in bfloat16 or wider, within the bound.
No kernel may reach another device: no remote copies, remote signals or barrier semaphores. Data moves between devices by JAX's collectives and lax.ppermute only.
A program may use at most 128 MiB of HBM per device.

```python
import math
import jax
import jax.numpy as jnp
from jax import lax

D = 4096
QHEADS = 32
KVHEADS = 8
HEAD = 128
UNIT = 32
DOC_UNITS = 8
U_DEV = 8
DOCS = 8
TOKENS = 2048
N_DP = 8


def draw_pair(key):
    base = jax.random.fold_in(key, 31)
    query_key, key_key = jax.random.split(base, 2)
    keys = jax.random.normal(key_key, (TOKENS, KVHEADS * HEAD), jnp.float32)
    queries = jax.random.normal(query_key, (TOKENS, QHEADS * HEAD), jnp.float32)
    return (queries, keys)


def draw_saved_query(key, part):
    return draw_pair(key)[0].astype(jnp.bfloat16)


def draw_saved_key(key, part):
    return draw_pair(key)[1].astype(jnp.bfloat16)


def draw_routing(key):
    base = jax.random.fold_in(key, 57)
    first, second, third, fourth, fifth = jax.random.split(base, 5)
    server_count = TOKENS // (UNIT * U_DEV)
    server_order = jax.random.permutation(first, server_count)
    trunk_order = jax.random.permutation(second, server_count)
    offsets = jax.random.permutation(third, server_count)[:U_DEV]
    ranks = jax.random.randint(fourth, (server_count, U_DEV), 0, 1 << 20) * U_DEV + jnp.arange(U_DEV)[None, :]
    slot_of = jnp.argsort(ranks, axis=1)
    servers = server_order[(trunk_order[:, None] + offsets[slot_of]) % server_count]
    place_ranks = jax.random.randint(fifth, (server_count, U_DEV), 0, 1 << 20) * U_DEV + jnp.arange(U_DEV)[None, :]
    place_table = jnp.argsort(place_ranks, axis=1)
    places = place_table[servers, slot_of]
    return (servers.reshape(-1).astype(jnp.int32), places.reshape(-1).astype(jnp.int32))


def draw_unit_server(key, part):
    return draw_routing(key)[0]


def draw_unit_place(key, part):
    return draw_routing(key)[1]


def plant(values, key, smallest, top_value):
    spot = [jax.random.randint(jax.random.fold_in(key, axis), (), 0, length) for axis, length in enumerate(values.shape)]
    longest = values.shape.index(max(values.shape))
    neighbour = spot[:longest] + [(spot[longest] + 1) % values.shape[longest]] + spot[longest + 1:]
    return values.at[tuple(spot)].set(smallest).at[tuple(neighbour)].set(top_value)


def block_levels(stream_key, dims, cuts, smallest, top_value):
    def one(axis_at, shards_of):
        draws = jax.random.uniform(jax.random.fold_in(jax.random.fold_in(stream_key, 6), axis_at), (shards_of,), jnp.float32, smallest / len(cuts), top_value / len(cuts))
        return jnp.repeat(jnp.exp(draws), dims[axis_at] // shards_of).reshape((-1,) + (1,) * (len(dims) - axis_at - 1))

    factor_of = one(*cuts[0])
    for cut in cuts[1:]:
        factor_of = factor_of * one(*cut)
    return factor_of


def scatter_about(own_key, shape, deviation, most, cuts=(), kind=jnp.bfloat16):
    array = deviation * jax.random.normal(own_key, shape, jnp.float32)
    if cuts:
        array = array * block_levels(own_key, shape, cuts, -0.22, 0.18)
    return jnp.clip(array, -most, most).astype(kind)


def setup_inputs(seed: int = 0) -> dict:
    key_list = jax.random.split(jax.random.key(seed), 11)
    saved_query = draw_saved_query(jax.random.fold_in(key_list[10], 71), 0)
    saved_key = draw_saved_key(jax.random.fold_in(key_list[10], 71), 0)
    saved_value = scatter_about(key_list[2], (TOKENS, KVHEADS * HEAD), 1.0, 6.0, ((0, 8), (1, 4)))
    grad_output = scatter_about(key_list[3], (TOKENS, QHEADS * HEAD), 4.0, 24.0, ((0, 8), (1, 4)))
    unit_server = draw_unit_server(jax.random.fold_in(key_list[10], 71), 0)
    unit_place = draw_unit_place(jax.random.fold_in(key_list[10], 71), 0)
    doc_length = plant(jax.random.randint(key_list[6], (DOCS,), 1, DOC_UNITS * UNIT + 1), jax.random.fold_in(key_list[6], 1), 1, DOC_UNITS * UNIT).astype(jnp.int32)
    query_weight = scatter_about(key_list[7], (D, QHEADS * HEAD), ((QHEADS + 2 * KVHEADS) * HEAD) ** -0.5, 0.078125, ((1, 4),))
    key_weight = scatter_about(key_list[8], (D, KVHEADS * HEAD), ((QHEADS + 2 * KVHEADS) * HEAD) ** -0.5, 0.078125, ((1, 4),))
    value_weight = scatter_about(key_list[9], (D, KVHEADS * HEAD), ((QHEADS + 2 * KVHEADS) * HEAD) ** -0.5, 0.078125, ((1, 4),))
    return {"saved_query": saved_query, "saved_key": saved_key, "saved_value": saved_value, "grad_output": grad_output, "unit_server": unit_server, "unit_place": unit_place, "doc_length": doc_length, "query_weight": query_weight, "key_weight": key_weight, "value_weight": value_weight}


def doc_backward(doc_query, doc_key, doc_value, doc_grad, length):
    block_rows = doc_query.shape[0]
    group_size = QHEADS // KVHEADS
    score_scale = 1.0 / math.sqrt(HEAD)
    highest = lax.Precision.HIGHEST
    rows_index = jnp.arange(block_rows, dtype=jnp.int32)
    live_rows = (rows_index < length).astype(doc_grad.dtype)
    masked = (doc_grad * live_rows[:, None]).astype(jnp.float32).reshape(block_rows, KVHEADS, group_size, HEAD)
    queries = doc_query.astype(jnp.float32).reshape(block_rows, KVHEADS, group_size, HEAD)
    keys = doc_key.astype(jnp.float32).reshape(block_rows, KVHEADS, HEAD)
    values = doc_value.astype(jnp.float32).reshape(block_rows, KVHEADS, HEAD)
    allowed = (rows_index[None, :] <= rows_index[:, None]) & (rows_index[None, :] < length)
    scores = jnp.einsum('ikgd,jkd->kgij', queries, keys, precision=highest) * score_scale
    scores = jnp.where(allowed, scores, -1e+30)
    row_peak = lax.optimization_barrier(jnp.max(scores, axis=-1, keepdims=True))
    expanded = jnp.where(allowed, jnp.exp(scores - row_peak), 0.0)
    attention = expanded / lax.optimization_barrier(jnp.sum(expanded, axis=-1, keepdims=True))
    attention_low = lax.optimization_barrier(attention.astype(jnp.bfloat16)).astype(jnp.float32)
    attended = jnp.einsum('kgij,jkd->ikgd', attention_low, values, precision=highest)
    row_delta = lax.optimization_barrier(jnp.sum(masked * attended, axis=-1))
    prob_grad = jnp.einsum('ikgd,jkd->kgij', masked, values, precision=highest)
    score_grad = attention * (prob_grad - jnp.transpose(row_delta, (1, 2, 0))[..., None])
    score_low = lax.optimization_barrier(score_grad.astype(jnp.bfloat16)).astype(jnp.float32)
    query_grad = jnp.einsum('kgij,jkd->ikgd', score_low, keys, precision=highest) * score_scale
    key_grad = jnp.einsum('kgij,ikgd->jkd', score_low, queries, precision=highest) * score_scale
    value_grad = jnp.einsum('kgij,ikgd->jkd', attention_low, masked, precision=highest)
    return (query_grad.reshape(block_rows, QHEADS * HEAD).astype(jnp.bfloat16), key_grad.reshape(block_rows, KVHEADS * HEAD).astype(jnp.bfloat16), value_grad.reshape(block_rows, KVHEADS * HEAD).astype(jnp.bfloat16))

def reference(saved_query, saved_key, saved_value, grad_output, unit_server, unit_place, doc_length, query_weight, key_weight, value_weight):
    unit_count = N_DP * U_DEV
    block_rows = DOC_UNITS * UNIT
    target = (unit_server * U_DEV + unit_place).astype(jnp.int32)

    def to_docs(tensor):
        columns = tensor.shape[1]
        pieces = tensor.reshape(unit_count, UNIT, columns)
        ordered = jnp.zeros_like(pieces).at[target].set(pieces)
        return ordered.reshape(unit_count // DOC_UNITS, block_rows, columns)

    def one_doc(element):
        return doc_backward(element[0], element[1], element[2], element[3], element[4])
    grads = lax.map(one_doc, (to_docs(saved_query), to_docs(saved_key), to_docs(saved_value), to_docs(grad_output), doc_length.astype(jnp.int32)))

    def to_tokens(tensor):
        columns = tensor.shape[2]
        pieces = tensor.reshape(unit_count, UNIT, columns)
        return pieces[target].reshape(unit_count * UNIT, columns)
    numbers = (((1,), (1,)), ((), ()))
    summed = lax.dot_general(to_tokens(grads[0]), query_weight, numbers, preferred_element_type=jnp.float32)
    summed = summed + lax.dot_general(to_tokens(grads[1]), key_weight, numbers, preferred_element_type=jnp.float32)
    summed = summed + lax.dot_general(to_tokens(grads[2]), value_weight, numbers, preferred_element_type=jnp.float32)
    return summed
```

```python
import functools
import math

import jax
import jax.numpy as jnp
from jax import lax
from jax.experimental import pallas as pl
from jax.experimental.pallas import tpu as pltpu
from jax.sharding import PartitionSpec as P

HEAD = 128
DOC_UNITS = 8
LANES = 128


def pack_kernel(server_ref, place_ref, q_ref, k_ref, v_ref, g_ref, out_ref):
    units = out_ref.shape[0]
    unit_rows = out_ref.shape[1]
    for u in range(units):
        slot = server_ref[u]
        rows = pl.ds(u * unit_rows, unit_rows)
        at = 0
        for ref in (q_ref, k_ref, v_ref, g_ref):
            width = ref.shape[1]
            out_ref[slot, :, at : at + width] = ref[rows, :]
            at += width
        place = jnp.full((unit_rows, LANES), place_ref[u], jnp.int32)
        out_ref[slot, :, at : at + LANES] = place.astype(jnp.float32).astype(out_ref.dtype)


def pack(unit_server, unit_place, q, k, v, g):
    units = unit_server.shape[0]
    width = q.shape[1] + k.shape[1] + v.shape[1] + g.shape[1] + LANES
    smem = pl.BlockSpec(memory_space=pltpu.SMEM)
    vmem = pl.BlockSpec(memory_space=pltpu.VMEM)
    return pl.pallas_call(
        pack_kernel,
        out_shape=jax.ShapeDtypeStruct((units, q.shape[0] // units, width), q.dtype),
        in_specs=[smem, smem, vmem, vmem, vmem, vmem],
        out_specs=vmem,
        name="pack",
    )(unit_server, unit_place, q, k, v, g)


NT = (((1,), (1,)), ((), ()))
TN = (((0,), (0,)), ((), ()))


def dot(a, b, numbers):
    return lax.dot_general(a, b, numbers, preferred_element_type=jnp.float32)


def server_kernel(
    kv_heads,
    tile,
    length_ref,
    arrived_ref,
    qw_hbm,
    kw_hbm,
    vw_hbm,
    out_hbm,
    qw,
    kw,
    vw,
    grads,
    partial,
    in_sems,
    out_sems,
):
    doc_count = length_ref.shape[0]
    slots, unit_rows, _ = arrived_ref.shape
    block_rows = slots * unit_rows // doc_count
    doc_slots = slots // doc_count
    parts = out_hbm.shape[1]
    part_width = out_hbm.shape[3]
    q_width = qw.shape[1]
    kv_width = kw.shape[1]
    group = q_width // kv_width
    scale = 1.0 / math.sqrt(HEAD)

    def weight_copies(part):
        rows = pl.ds(part * part_width, part_width)
        return [
            pltpu.make_async_copy(hbm.at[rows], vmem.at[rows], in_sems.at[part, n])
            for n, (hbm, vmem) in enumerate(((qw_hbm, qw), (kw_hbm, kw), (vw_hbm, vw)))
        ]

    for part in range(parts):
        for copy in weight_copies(part):
            copy.start()

    for doc in range(doc_count):
        here = pl.ds(doc * doc_slots, doc_slots)
        rows = pl.ds(doc * block_rows, block_rows)
        length = length_ref[doc].astype(jnp.float32)

        def load(at, width):
            return arrived_ref[here, :, at : at + width].reshape(block_rows, width)

        at_place = 2 * (q_width + kv_width)
        place = load(at_place, LANES).astype(jnp.float32)
        row = lax.broadcasted_iota(jnp.int32, (block_rows, LANES), 0).astype(jnp.float32)
        slot = jnp.floor(row * (1.0 / unit_rows))
        place = place - DOC_UNITS * jnp.floor(place * (1.0 / DOC_UNITS))
        position = place * unit_rows + (row - slot * unit_rows)
        query_at = position[:, :1]
        key_at = jnp.transpose(position)[:1, :]
        allowed = (key_at <= query_at) & (key_at < length)
        live = query_at < length
        for kv in range(kv_heads):
            keys = load(q_width + kv * HEAD, HEAD)
            values = load(q_width + kv_width + kv * HEAD, HEAD)
            key_grad = None
            value_grad = None
            for h in range(kv * group, (kv + 1) * group):
                queries = load(h * HEAD, HEAD)
                outer = load(q_width + 2 * kv_width + h * HEAD, HEAD)
                masked = jnp.where(live, outer.astype(jnp.float32), 0.0).astype(jnp.bfloat16)
                scores = dot(queries, keys, NT) * scale
                scores = jnp.where(allowed, scores, -1e30)
                peak = jnp.max(scores, axis=1, keepdims=True)
                expanded = jnp.where(allowed, jnp.exp(scores - peak), 0.0)
                probs = expanded * (1.0 / jnp.sum(expanded, axis=1, keepdims=True))
                probs_low = probs.astype(jnp.bfloat16)
                prob_grad = dot(masked, values, NT)
                delta = jnp.sum(probs_low.astype(jnp.float32) * prob_grad, axis=1, keepdims=True)
                score_low = (probs * (prob_grad - delta)).astype(jnp.bfloat16)
                query_grad = dot(score_low, keys, (((1,), (0,)), ((), ()))) * scale
                grads[rows, h * HEAD : (h + 1) * HEAD] = query_grad.astype(jnp.bfloat16)
                dk = dot(score_low, queries, TN)
                dv = dot(probs_low, masked, TN)
                key_grad = dk if key_grad is None else key_grad + dk
                value_grad = dv if value_grad is None else value_grad + dv
            at = q_width + kv * HEAD
            grads[rows, at : at + HEAD] = (key_grad * scale).astype(jnp.bfloat16)
            at = q_width + kv_width + kv * HEAD
            grads[rows, at : at + HEAD] = value_grad.astype(jnp.bfloat16)

    def out_copy(part):
        return pltpu.make_async_copy(
            partial.at[part], out_hbm.at[:, part], out_sems.at[part]
        )

    for part in range(parts):
        for copy in weight_copies(part):
            copy.wait()
        for at in range(0, part_width, tile):
            columns = pl.ds(part * part_width + at, tile)
            total = dot(grads[:, :q_width], qw[columns, :], NT)
            total = total + dot(grads[:, q_width : q_width + kv_width], kw[columns, :], NT)
            total = total + dot(grads[:, q_width + kv_width :], vw[columns, :], NT)
            partial[part, :, :, at : at + tile] = total.astype(jnp.bfloat16).reshape(
                slots, unit_rows, tile
            )
        out_copy(part).start()
    for part in range(parts):
        out_copy(part).wait()


def serve(doc_length, arrived, qw, kw, vw, parts):
    slots, unit_rows, _ = arrived.shape
    width = qw.shape[0]
    part_width = width // parts
    kv_heads = kw.shape[1] // HEAD
    rows = slots * unit_rows
    hbm = pl.BlockSpec(memory_space=pl.ANY)
    bf16 = jnp.bfloat16
    return pl.pallas_call(
        functools.partial(server_kernel, kv_heads, min(256, part_width)),
        out_shape=jax.ShapeDtypeStruct((slots, parts, unit_rows, part_width), bf16),
        in_specs=[
            pl.BlockSpec(memory_space=pltpu.SMEM),
            pl.BlockSpec(memory_space=pltpu.VMEM),
            hbm,
            hbm,
            hbm,
        ],
        out_specs=hbm,
        scratch_shapes=[
            pltpu.VMEM(qw.shape, bf16),
            pltpu.VMEM(kw.shape, bf16),
            pltpu.VMEM(vw.shape, bf16),
            pltpu.VMEM((rows, qw.shape[1] + 2 * kw.shape[1]), bf16),
            pltpu.VMEM((parts, slots, unit_rows, part_width), bf16),
            pltpu.SemaphoreType.DMA((parts, 3)),
            pltpu.SemaphoreType.DMA((parts,)),
        ],
        compiler_params=pltpu.CompilerParams(vmem_limit_bytes=56 << 20),
        name="serve",
    )(doc_length, arrived, qw, kw, vw)


def gather_sum_kernel(server_ref, back_ref, out_ref):
    total = back_ref[0].astype(jnp.float32)
    for part in range(1, back_ref.shape[0]):
        total = total + back_ref[part].astype(jnp.float32)
    out_ref[...] = total


def gather_sum(unit_server, back):
    _, parts, unit_rows, width = back.shape
    units = unit_server.shape[0]
    return pl.pallas_call(
        gather_sum_kernel,
        out_shape=jax.ShapeDtypeStruct((units * unit_rows, width), jnp.float32),
        grid_spec=pltpu.PrefetchScalarGridSpec(
            num_scalar_prefetch=1,
            grid=(units,),
            in_specs=[
                pl.BlockSpec(
                    (pl.Squeezed(), parts, unit_rows, width), lambda u, server: (server[u], 0, 0, 0)
                )
            ],
            out_specs=pl.BlockSpec((unit_rows, width), lambda u, server: (u, 0)),
        ),
        name="gather_sum",
    )(unit_server, back)


def local(
    saved_query,
    saved_key,
    saved_value,
    grad_output,
    unit_server,
    unit_place,
    doc_length,
    query_weight,
    key_weight,
    value_weight,
):
    servers = lax.axis_size("dp")
    parts = lax.axis_size("mp")
    doc_count = doc_length.shape[0]
    outgoing = pack(unit_server, unit_place, saved_query, saved_key, saved_value, grad_output)
    arrived = lax.all_to_all(outgoing, "dp", split_axis=0, concat_axis=0, tiled=True)
    slots, unit_rows, _ = arrived.shape
    order = None
    if doc_count > 1:
        place = arrived[:, 0, -1].astype(jnp.int32)
        order = jnp.argsort(place)
        arrived = arrived[order]
    partial = serve(doc_length, arrived, query_weight, key_weight, value_weight, parts)
    if order is not None:
        partial = partial[place]
    width = partial.shape[-1]
    back = lax.all_to_all(
        partial.reshape(slots * parts, unit_rows, width),
        ("dp", "mp"),
        split_axis=0,
        concat_axis=0,
        tiled=True,
    )
    return gather_sum(unit_server, back.reshape(servers, parts, unit_rows, width))


def solution(mesh):
    placed = (
        P("dp", "mp"),
        P("dp", "mp"),
        P("dp", "mp"),
        P("dp", "mp"),
        P("dp"),
        P("dp"),
        P("dp"),
        P(None, "mp"),
        P(None, "mp"),
        P(None, "mp"),
    )
    return jax.shard_map(
        local, mesh=mesh, in_specs=placed, out_specs=P("dp", "mp"), check_vma=False
    )
```

```python
import functools
import math

import jax
import jax.numpy as jnp
from jax import lax
from jax.experimental import pallas as pl
from jax.experimental.pallas import tpu as pltpu
from jax.sharding import PartitionSpec as P

HEAD = 128
DOC_UNITS = 8
LANES = 128
TILE = 128
PACK_VMEM = 32 << 20
SERVE_VMEM = 50 << 20
SUM_VMEM = 12 << 20


def pack_kernel(server_ref, place_ref, q_ref, k_ref, v_ref, g_ref, out_ref):
    units = out_ref.shape[0]
    unit_rows = out_ref.shape[1]
    for u in range(units):
        slot = server_ref[u]
        rows = pl.ds(u * unit_rows, unit_rows)
        at = 0
        for ref in (q_ref, k_ref, v_ref, g_ref):
            width = ref.shape[1]
            out_ref[slot, :, at : at + width] = ref[rows, :]
            at += width
        place = jnp.full((unit_rows, LANES), place_ref[u], jnp.int32)
        out_ref[slot, :, at : at + LANES] = place.astype(jnp.float32).astype(out_ref.dtype)


def pack(unit_server, unit_place, q, k, v, g):
    units = unit_server.shape[0]
    width = q.shape[1] + k.shape[1] + v.shape[1] + g.shape[1] + LANES
    smem = pl.BlockSpec(memory_space=pltpu.SMEM)
    vmem = pl.BlockSpec(memory_space=pltpu.VMEM)
    return pl.pallas_call(
        pack_kernel,
        out_shape=jax.ShapeDtypeStruct((units, q.shape[0] // units, width), q.dtype),
        in_specs=[smem, smem, vmem, vmem, vmem, vmem],
        out_specs=vmem,
        compiler_params=pltpu.CompilerParams(vmem_limit_bytes=PACK_VMEM),
        name="pack",
    )(unit_server, unit_place, q, k, v, g)


NN = (((1,), (0,)), ((), ()))
NT = (((1,), (1,)), ((), ()))
TN = (((0,), (0,)), ((), ()))


def dot(a, b, numbers):
    return lax.dot_general(a, b, numbers, preferred_element_type=jnp.float32)


def server_kernel(
    kv_heads,
    tile,
    length_ref,
    arrived_ref,
    qw_hbm,
    kw_hbm,
    vw_hbm,
    out_ref,
    qw,
    kw,
    vw,
    grads,
    bias,
    queries,
    masked,
    probs_low,
    score_low,
    in_sems,
):
    doc_count = length_ref.shape[0]
    slots, unit_rows, _ = arrived_ref.shape
    block_rows = slots * unit_rows // doc_count
    doc_slots = slots // doc_count
    parts = out_ref.shape[1]
    part_width = out_ref.shape[3]
    q_width = qw.shape[1]
    kv_width = kw.shape[1]
    group = q_width // kv_width
    scale = 1.0 / math.sqrt(HEAD)

    def weight_copies(part):
        rows = pl.ds(part * part_width, part_width)
        return [
            pltpu.make_async_copy(hbm.at[rows], vmem.at[rows], in_sems.at[part, n])
            for n, (hbm, vmem) in enumerate(((qw_hbm, qw), (kw_hbm, kw), (vw_hbm, vw)))
        ]

    for part in range(parts):
        for copy in weight_copies(part):
            copy.start()

    for doc in range(doc_count):
        here = pl.ds(doc * doc_slots, doc_slots)
        rows = pl.ds(doc * block_rows, block_rows)
        length = length_ref[doc].astype(jnp.float32)

        def load(at, width):
            return arrived_ref[here, :, at : at + width].reshape(block_rows, width)

        at_place = 2 * (q_width + kv_width)
        place = load(at_place, LANES).astype(jnp.float32)
        row = lax.broadcasted_iota(jnp.int32, (block_rows, LANES), 0).astype(jnp.float32)
        slot = jnp.floor(row * (1.0 / unit_rows))
        place = place - DOC_UNITS * jnp.floor(place * (1.0 / DOC_UNITS))
        position = place * unit_rows + (row - slot * unit_rows)
        live = position < length
        key_at = position[:, :1]
        query_at = jnp.transpose(position)[:1, :]
        allowed = (key_at <= query_at) & (key_at < length)
        bias[...] = jnp.where(allowed, 0.0, -1e30)
        tiles = block_rows // TILE
        for kv in range(kv_heads):
            keys = load(q_width + kv * HEAD, HEAD)
            values = load(q_width + kv_width + kv * HEAD, HEAD)
            for h in range(group):
                head = kv * group + h
                here_rows = slice(h * block_rows, (h + 1) * block_rows)
                queries[here_rows, :] = load(head * HEAD, HEAD)
                outer = load(q_width + 2 * kv_width + head * HEAD, HEAD).astype(jnp.float32)
                masked[here_rows, :] = jnp.where(live, outer, 0.0).astype(jnp.bfloat16)
            for t in range(group * tiles):
                at = t * TILE
                within = (t % tiles) * TILE
                scores = dot(keys, queries[at : at + TILE, :], NT) * scale
                scores = scores + bias[:, within : within + TILE]
                peak = jnp.max(scores, axis=0, keepdims=True)
                expanded = jnp.exp(scores - peak)
                probs = expanded * (1.0 / jnp.sum(expanded, axis=0, keepdims=True))
                low = probs.astype(jnp.bfloat16)
                probs_low[:, at : at + TILE] = low
                prob_grad = dot(values, masked[at : at + TILE, :], NT)
                delta = jnp.sum(low.astype(jnp.float32) * prob_grad, axis=0, keepdims=True)
                score_low[:, at : at + TILE] = (probs * (prob_grad - delta)).astype(jnp.bfloat16)
            at = q_width + kv * HEAD
            grads[rows, at : at + HEAD] = (
                dot(score_low[...], queries[...], NN) * scale
            ).astype(jnp.bfloat16)
            at = q_width + kv_width + kv * HEAD
            grads[rows, at : at + HEAD] = dot(probs_low[...], masked[...], NN).astype(jnp.bfloat16)
            for h in range(group):
                at = (kv * group + h) * HEAD
                grads[rows, at : at + HEAD] = (
                    dot(score_low[:, h * block_rows : (h + 1) * block_rows], keys, TN) * scale
                ).astype(jnp.bfloat16)

    for part in range(parts):
        for copy in weight_copies(part):
            copy.wait()
        for at in range(0, part_width, tile):
            columns = pl.ds(part * part_width + at, tile)
            total = dot(grads[:, :q_width], qw[columns, :], NT)
            total = total + dot(grads[:, q_width : q_width + kv_width], kw[columns, :], NT)
            total = total + dot(grads[:, q_width + kv_width :], vw[columns, :], NT)
            out_ref[:, part, :, at : at + tile] = total.astype(jnp.bfloat16).reshape(
                slots, unit_rows, tile
            )


def serve(doc_length, arrived, qw, kw, vw, parts):
    slots, unit_rows, _ = arrived.shape
    width = qw.shape[0]
    part_width = width // parts
    kv_heads = kw.shape[1] // HEAD
    rows = slots * unit_rows
    block = rows // doc_length.shape[0]
    group = qw.shape[1] // kw.shape[1]
    hbm = pl.BlockSpec(memory_space=pltpu.HBM)
    bf16 = jnp.bfloat16
    return pl.pallas_call(
        functools.partial(server_kernel, kv_heads, min(256, part_width)),
        out_shape=jax.ShapeDtypeStruct((slots, parts, unit_rows, part_width), bf16),
        in_specs=[
            pl.BlockSpec(memory_space=pltpu.SMEM),
            pl.BlockSpec(memory_space=pltpu.VMEM),
            hbm,
            hbm,
            hbm,
        ],
        out_specs=pl.BlockSpec(memory_space=pltpu.VMEM),
        scratch_shapes=[
            pltpu.VMEM(qw.shape, bf16),
            pltpu.VMEM(kw.shape, bf16),
            pltpu.VMEM(vw.shape, bf16),
            pltpu.VMEM((rows, qw.shape[1] + 2 * kw.shape[1]), bf16),
            pltpu.VMEM((block, block), jnp.float32),
            pltpu.VMEM((group * block, HEAD), bf16),
            pltpu.VMEM((group * block, HEAD), bf16),
            pltpu.VMEM((block, group * block), bf16),
            pltpu.VMEM((block, group * block), bf16),
            pltpu.SemaphoreType.DMA((parts, 3)),
        ],
        compiler_params=pltpu.CompilerParams(vmem_limit_bytes=SERVE_VMEM),
        name="serve",
    )(doc_length, arrived, qw, kw, vw)


def gather_sum_kernel(server_ref, back_ref, out_hbm, total, sems):
    units, unit_rows, _ = total.shape

    def out_copy(u):
        return pltpu.make_async_copy(
            total.at[u], out_hbm.at[pl.ds(u * unit_rows, unit_rows)], sems.at[u]
        )

    for u in range(units):
        server = server_ref[u]
        summed = back_ref[server, 0].astype(jnp.float32)
        for part in range(1, back_ref.shape[1]):
            summed = summed + back_ref[server, part].astype(jnp.float32)
        total[u] = summed
        out_copy(u).start()
    for u in range(units):
        out_copy(u).wait()


def gather_sum(unit_server, back):
    _, _, unit_rows, width = back.shape
    units = unit_server.shape[0]
    return pl.pallas_call(
        gather_sum_kernel,
        out_shape=jax.ShapeDtypeStruct((units * unit_rows, width), jnp.float32),
        in_specs=[
            pl.BlockSpec(memory_space=pltpu.SMEM),
            pl.BlockSpec(memory_space=pltpu.VMEM),
        ],
        out_specs=pl.BlockSpec(memory_space=pl.ANY),
        scratch_shapes=[
            pltpu.VMEM((units, unit_rows, width), jnp.float32),
            pltpu.SemaphoreType.DMA((units,)),
        ],
        compiler_params=pltpu.CompilerParams(vmem_limit_bytes=SUM_VMEM),
        name="gather_sum",
    )(unit_server, back)


def local(
    saved_query,
    saved_key,
    saved_value,
    grad_output,
    unit_server,
    unit_place,
    doc_length,
    query_weight,
    key_weight,
    value_weight,
):
    servers = lax.axis_size("dp")
    parts = lax.axis_size("mp")
    doc_count = doc_length.shape[0]
    outgoing = pack(unit_server, unit_place, saved_query, saved_key, saved_value, grad_output)
    arrived = lax.all_to_all(outgoing, "dp", split_axis=0, concat_axis=0, tiled=True)
    slots, unit_rows, _ = arrived.shape
    order = None
    if doc_count > 1:
        place = arrived[:, 0, -1].astype(jnp.int32)
        order = jnp.argsort(place)
        arrived = arrived[order]
    partial = serve(doc_length, arrived, query_weight, key_weight, value_weight, parts)
    if order is not None:
        partial = partial[place]
    width = partial.shape[-1]
    back = lax.all_to_all(
        partial.reshape(slots * parts, unit_rows, width),
        ("dp", "mp"),
        split_axis=0,
        concat_axis=0,
        tiled=True,
    )
    return gather_sum(unit_server, back.reshape(servers, parts, unit_rows, width))


def solution(mesh):
    placed = (
        P("dp", "mp"),
        P("dp", "mp"),
        P("dp", "mp"),
        P("dp", "mp"),
        P("dp"),
        P("dp"),
        P("dp"),
        P(None, "mp"),
        P(None, "mp"),
        P(None, "mp"),
    )
    return jax.shard_map(
        local, mesh=mesh, in_specs=placed, out_specs=P("dp", "mp"), check_vma=False
    )
```

```python
import functools
import math

import jax
import jax.numpy as jnp
from jax import lax
from jax.experimental import pallas as pl
from jax.experimental.pallas import tpu as pltpu
from jax.sharding import PartitionSpec as P

HEAD = 128
DOC_UNITS = 8
LANES = 128
TILE = 128
COLUMNS = 256
PACK_VMEM = 60 << 20
SERVE_VMEM = 50 << 20
REST_VMEM = 52 << 20
SUM_VMEM = 12 << 20


NN = (((1,), (0,)), ((), ()))
NT = (((1,), (1,)), ((), ()))
TN = (((0,), (0,)), ((), ()))

SMEM = pl.BlockSpec(memory_space=pltpu.SMEM)
VMEM = pl.BlockSpec(memory_space=pltpu.VMEM)
HBM = pl.BlockSpec(memory_space=pltpu.HBM)
BF16 = jnp.bfloat16


def dot(a, b, numbers):
    return lax.dot_general(a, b, numbers, preferred_element_type=jnp.float32)


def find_units(server_ref, unit_of, servers):
    me = lax.axis_index("dp")
    for u in range(servers):
        unit_of[jnp.bitwise_xor(server_ref[u], me)] = u


def pack_kernel(server_ref, place_ref, q_ref, k_ref, v_ref, g_ref, *rest):
    out_refs, unit_of = rest[:-1], rest[-1]
    unit_rows = out_refs[0].shape[0]
    find_units(server_ref, unit_of, len(out_refs))
    for k, out_ref in enumerate(out_refs):
        u = unit_of[k]
        rows = pl.ds(pl.multiple_of(u * unit_rows, unit_rows), unit_rows)
        at = 0
        for ref in (q_ref, k_ref, v_ref, g_ref):
            width = ref.shape[1]
            out_ref[:, at : at + width] = ref[rows, :]
            at += width
        place = jnp.full((unit_rows, LANES), place_ref[u], jnp.int32)
        out_ref[:, at : at + LANES] = place.astype(jnp.float32).astype(out_ref.dtype)


def pack(unit_server, unit_place, q, k, v, g):
    units = unit_server.shape[0]
    width = q.shape[1] + k.shape[1] + v.shape[1] + g.shape[1] + LANES
    piece = jax.ShapeDtypeStruct((q.shape[0] // units, width), q.dtype)
    return pl.pallas_call(
        pack_kernel,
        out_shape=[piece] * units,
        in_specs=[SMEM, SMEM, VMEM, VMEM, VMEM, VMEM],
        out_specs=[VMEM] * units,
        scratch_shapes=[pltpu.SMEM((units,), jnp.int32)],
        compiler_params=pltpu.CompilerParams(vmem_limit_bytes=PACK_VMEM),
        name="pack",
    )(unit_server, unit_place, q, k, v, g)


def weight_copies(hbm_refs, vmem_refs, sems, n, r, part_width):
    part = jnp.bitwise_xor(lax.axis_index("mp"), r)
    source = pl.ds(pl.multiple_of(part * part_width, part_width), part_width)
    return [
        pltpu.make_async_copy(hbm.at[source], vmem.at[n], sems.at[n, i])
        for i, (hbm, vmem) in enumerate(zip(hbm_refs, vmem_refs))
    ]


def project(grads, weights, n, store, part_width):
    tile = min(COLUMNS, part_width)
    for at in range(0, part_width, tile):
        total = None
        left = 0
        for weight in weights:
            width = weight.shape[2]
            term = dot(grads[:, left : left + width], weight[n, at : at + tile, :], NT)
            total = term if total is None else total + term
            left += width
        store(at, tile, total.astype(BF16))


def serve_kernel(kv_heads, parts, sizes, length_ref, *refs):
    servers = sum(sizes)
    arrived = refs[:servers]
    hbm_refs = refs[servers : servers + 3]
    grads = refs[servers + 3]
    out_refs = refs[servers + 4 : servers + 4 + len(sizes)]
    qw, kw, vw, bias, queries, masked, probs_low, score_low, sems = refs[servers + 4 + len(sizes) :]
    unit_rows = arrived[0].shape[0]
    rows = servers * unit_rows
    doc_count = length_ref.shape[0]
    part_width = qw.shape[1]
    q_width = qw.shape[2]
    kv_width = kw.shape[2]
    group = q_width // kv_width
    scale = 1.0 / math.sqrt(HEAD)

    def copies(n):
        return weight_copies(hbm_refs, (qw, kw, vw), sems, n, parts[n], part_width)

    for n in range(len(parts)):
        for copy in copies(n):
            copy.start()

    def load(at, width):
        return jnp.concatenate([ref[:, at : at + width] for ref in arrived], axis=0)

    place = load(2 * (q_width + kv_width), LANES).astype(jnp.float32)
    row = lax.broadcasted_iota(jnp.int32, (rows, LANES), 0).astype(jnp.float32)
    doc = jnp.floor(place * (1.0 / DOC_UNITS))
    position = (place - DOC_UNITS * doc) * unit_rows
    position = position + (row - unit_rows * jnp.floor(row * (1.0 / unit_rows)))
    length = jnp.full((rows, LANES), length_ref[0], jnp.int32).astype(jnp.float32)
    for d in range(1, doc_count):
        length = jnp.where(doc == d, length_ref[d].astype(jnp.float32), length)
    live = position < length
    key_at = jnp.where(live, position, 1e9)[:, :1]
    allowed = key_at <= jnp.transpose(position)[:1, :]
    if doc_count > 1:
        allowed = allowed & (doc[:, :1] == jnp.transpose(doc)[:1, :])
    bias[...] = jnp.where(allowed, 0.0, -1e30)
    tiles = rows // TILE
    for kv in range(kv_heads):
        keys = load(q_width + kv * HEAD, HEAD)
        values = load(q_width + kv_width + kv * HEAD, HEAD)
        for h in range(group):
            head = kv * group + h
            here = slice(h * rows, (h + 1) * rows)
            queries[here, :] = load(head * HEAD, HEAD)
            outer = load(q_width + 2 * kv_width + head * HEAD, HEAD).astype(jnp.float32)
            masked[here, :] = jnp.where(live, outer, 0.0).astype(BF16)
        for t in range(group * tiles):
            at = t * TILE
            within = (t % tiles) * TILE
            scores = dot(keys, queries[at : at + TILE, :], NT) * scale
            scores = scores + bias[:, within : within + TILE]
            peak = jnp.max(scores, axis=0, keepdims=True)
            expanded = jnp.exp(scores - peak)
            probs = expanded * (1.0 / jnp.sum(expanded, axis=0, keepdims=True))
            low = probs.astype(BF16)
            probs_low[:, at : at + TILE] = low
            prob_grad = dot(values, masked[at : at + TILE, :], NT)
            delta = jnp.sum(low.astype(jnp.float32) * prob_grad, axis=0, keepdims=True)
            score_low[:, at : at + TILE] = (probs * (prob_grad - delta)).astype(BF16)
        at = q_width + kv * HEAD
        grads[:, at : at + HEAD] = (dot(score_low[...], queries[...], NN) * scale).astype(BF16)
        at = q_width + kv_width + kv * HEAD
        grads[:, at : at + HEAD] = dot(probs_low[...], masked[...], NN).astype(BF16)
        for h in range(group):
            at = (kv * group + h) * HEAD
            grads[:, at : at + HEAD] = (
                dot(score_low[:, h * rows : (h + 1) * rows], keys, TN) * scale
            ).astype(BF16)

    for n in range(len(parts)):
        for copy in copies(n):
            copy.wait()

        def store(at, tile, value):
            first = 0
            for size, out_ref in zip(sizes, out_refs):
                piece = value[first * unit_rows : (first + size) * unit_rows, :]
                out_ref[n, :, :, at : at + tile] = piece.reshape(size, unit_rows, tile)
                first += size

        project(grads, (qw, kw, vw), n, store, part_width)


def weight_scratch(count, part_width, weights):
    return [pltpu.VMEM((count, part_width, w.shape[1]), BF16) for w in weights] + [
        pltpu.SemaphoreType.DMA((count, len(weights)))
    ]


def serve(doc_length, arrived, weights, parts, sizes, part_width):
    qw, kw, _ = weights
    unit_rows = arrived[0].shape[0]
    rows = unit_rows * len(arrived)
    group = qw.shape[1] // kw.shape[1]
    kv_heads = kw.shape[1] // HEAD
    width = qw.shape[1] + 2 * kw.shape[1]
    *buffers, sems = weight_scratch(len(parts), part_width, weights)
    flops = 2 * rows * width * part_width * len(parts)
    flops += 10 * rows * rows * qw.shape[1]
    return pl.pallas_call(
        functools.partial(serve_kernel, kv_heads, parts, sizes),
        out_shape=[jax.ShapeDtypeStruct((rows, width), BF16)]
        + [
            jax.ShapeDtypeStruct((len(parts), size, unit_rows, part_width), BF16)
            for size in sizes
        ],
        in_specs=[SMEM] + [VMEM] * len(arrived) + [HBM] * 3,
        out_specs=[VMEM] * (1 + len(sizes)),
        scratch_shapes=buffers
        + [
            pltpu.VMEM((rows, rows), jnp.float32),
            pltpu.VMEM((group * rows, HEAD), BF16),
            pltpu.VMEM((group * rows, HEAD), BF16),
            pltpu.VMEM((rows, group * rows), BF16),
            pltpu.VMEM((rows, group * rows), BF16),
            sems,
        ],
        compiler_params=pltpu.CompilerParams(vmem_limit_bytes=SERVE_VMEM),
        cost_estimate=pl.CostEstimate(flops=flops, bytes_accessed=0, transcendentals=0),
        name="serve",
    )(doc_length, *arrived, *weights)


def rest_kernel(parts, grads, qw_hbm, kw_hbm, vw_hbm, out_ref, qw, kw, vw, sems):
    part_width = qw.shape[1]
    _, slots, unit_rows, _ = out_ref.shape

    def copies(n):
        return weight_copies((qw_hbm, kw_hbm, vw_hbm), (qw, kw, vw), sems, n, parts[n], part_width)

    for n in range(len(parts)):
        for copy in copies(n):
            copy.start()
    for n in range(len(parts)):
        for copy in copies(n):
            copy.wait()

        def store(at, tile, value):
            out_ref[n, :, :, at : at + tile] = value.reshape(slots, unit_rows, tile)

        project(grads, (qw, kw, vw), n, store, part_width)


def rest(grads, weights, parts, slots, part_width):
    rows, width = grads.shape
    return pl.pallas_call(
        functools.partial(rest_kernel, parts),
        out_shape=jax.ShapeDtypeStruct((len(parts), slots, rows // slots, part_width), BF16),
        in_specs=[VMEM] + [HBM] * 3,
        out_specs=VMEM,
        scratch_shapes=weight_scratch(len(parts), part_width, weights),
        compiler_params=pltpu.CompilerParams(vmem_limit_bytes=REST_VMEM),
        cost_estimate=pl.CostEstimate(
            flops=2 * rows * width * part_width * len(parts), bytes_accessed=0, transcendentals=0
        ),
        name="rest",
    )(grads, *weights)


def combine_kernel(first, here_ref, there_ref, *out_refs):
    count, size = there_ref.shape[:2]
    for n in range(count):
        for i in range(size):
            total = here_ref[n, first + i].astype(jnp.float32)
            total = total + there_ref[n, i].astype(jnp.float32)
            out_refs[n * size + i][...] = total.astype(BF16)


def combine(here, there, first):
    count, size, unit_rows, width = there.shape
    outs = pl.pallas_call(
        functools.partial(combine_kernel, first),
        out_shape=[jax.ShapeDtypeStruct((unit_rows, width), BF16)] * (count * size),
        in_specs=[VMEM, VMEM],
        out_specs=[VMEM] * (count * size),
        compiler_params=pltpu.CompilerParams(vmem_limit_bytes=SERVE_VMEM),
        name="combine",
    )(here, there)
    return [outs[n * size : (n + 1) * size] for n in range(count)]


def sum_kernel(server_ref, *refs):
    out_hbm, total, unit_of, sems = refs[-4:]
    units, unit_rows, _ = total.shape
    near, far = refs[:units], refs[units : 2 * units]
    find_units(server_ref, unit_of, units)

    def out_copy(k):
        at = pl.multiple_of(unit_of[k] * unit_rows, unit_rows)
        return pltpu.make_async_copy(total.at[k], out_hbm.at[pl.ds(at, unit_rows)], sems.at[k])

    for k in range(units):
        total[k] = near[k][...].astype(jnp.float32) + far[k][...].astype(jnp.float32)
        out_copy(k).start()
    for k in range(units):
        out_copy(k).wait()


def final_sum(unit_server, near, far):
    units = len(near)
    unit_rows, width = near[0].shape
    return pl.pallas_call(
        sum_kernel,
        out_shape=jax.ShapeDtypeStruct((units * unit_rows, width), jnp.float32),
        in_specs=[SMEM] + [VMEM] * (2 * units),
        out_specs=pl.BlockSpec(memory_space=pl.ANY),
        scratch_shapes=[
            pltpu.VMEM((units, unit_rows, width), jnp.float32),
            pltpu.SMEM((units,), jnp.int32),
            pltpu.SemaphoreType.DMA((units,)),
        ],
        compiler_params=pltpu.CompilerParams(vmem_limit_bytes=SUM_VMEM),
        name="final_sum",
    )(unit_server, *near, *far)


def local(
    saved_query,
    saved_key,
    saved_value,
    grad_output,
    unit_server,
    unit_place,
    doc_length,
    query_weight,
    key_weight,
    value_weight,
):
    servers = lax.axis_size("dp")
    planes = lax.axis_size("mp")
    if servers & (servers - 1) or planes & (planes - 1) or planes < 4 or servers < 2:
        raise ValueError("mesh size")
    part_width = query_weight.shape[0] // planes
    weights = (query_weight, key_weight, value_weight)

    def dp_swap(value, k):
        return lax.ppermute(value, "dp", [(i, i ^ k) for i in range(servers)])

    def mp_swap(value, bit):
        return lax.ppermute(value, "mp", [(i, i ^ bit) for i in range(planes)])

    def both_swap(value, k, bit):
        pairs = [
            (d * planes + z, (d ^ k) * planes + (z ^ bit))
            for d in range(servers)
            for z in range(planes)
        ]
        return lax.ppermute(value, ("dp", "mp"), pairs)

    pieces = pack(unit_server, unit_place, saved_query, saved_key, saved_value, grad_output)
    arrived = [None] * servers
    arrived[0] = pieces[0]
    for k in range(servers - 1, 0, -1):
        arrived[k] = dp_swap(pieces[k], k)
    order = list(range(servers - 1, -1, -1))
    half = servers // 2
    groups = (order[half:], order[:half])
    sizes = tuple(len(g) for g in groups)
    odd = tuple(range(1, planes, 2))
    even = tuple(range(0, planes, 2))
    grads, *sent = serve(
        doc_length, [arrived[k] for k in groups[0] + groups[1]], weights, odd, sizes, part_width
    )
    crossed = []
    for i, value in enumerate(sent):
        with jax.named_scope(f"hop_{i}"):
            crossed.append(mp_swap(value, 1))
    kept = rest(grads, weights, even, servers, part_width)
    near = [None] * servers
    far = [None] * servers
    first = 0
    for i, (group, there) in enumerate(zip(groups, crossed)):
        outs = None
        if planes > 4:
            total = kept[:, first : first + len(group)] + there
            bit = 2
            while bit < planes // 2:
                total = total[0::2] + mp_swap(total[1::2], bit)
                bit *= 2
            outs = [[total[n, m] for m in range(len(group))] for n in range(2)]
        else:
            outs = combine(kept, there, first)
        first += len(group)
        with jax.named_scope(f"home_{i}"):
            for m, k in enumerate(group):
                far[k] = both_swap(outs[1][m], k, planes // 2)
                near[k] = dp_swap(outs[0][m], k) if k else outs[0][m]
    return final_sum(unit_server, near, far)


def solution(mesh):
    placed = (
        P("dp", "mp"),
        P("dp", "mp"),
        P("dp", "mp"),
        P("dp", "mp"),
        P("dp"),
        P("dp"),
        P("dp"),
        P(None, "mp"),
        P(None, "mp"),
        P(None, "mp"),
    )
    return jax.shard_map(
        local, mesh=mesh, in_specs=placed, out_specs=P("dp", "mp"), check_vma=False
    )
```

```python
import functools
import math

import jax
import jax.numpy as jnp
from jax import lax
from jax.experimental import pallas as pl
from jax.experimental.pallas import tpu as pltpu
from jax.sharding import PartitionSpec as P


HEAD = 128
DOC_UNITS = 8
LANES = 128
TILE = 128
CUTS = (2, 4, 6)
COLUMNS = 256
PACK_VMEM = 60 << 20
SERVE_VMEM = 50 << 20
REST_VMEM = 52 << 20
SUM_VMEM = 12 << 20


NN = (((1,), (0,)), ((), ()))
NT = (((1,), (1,)), ((), ()))
TN = (((0,), (0,)), ((), ()))

SMEM = pl.BlockSpec(memory_space=pltpu.SMEM)
VMEM = pl.BlockSpec(memory_space=pltpu.VMEM)
HBM = pl.BlockSpec(memory_space=pltpu.HBM)
BF16 = jnp.bfloat16


def dot(a, b, numbers):
    return lax.dot_general(a, b, numbers, preferred_element_type=jnp.float32)


def find_units(server_ref, unit_of, servers):
    me = lax.axis_index("dp")
    for u in range(servers):
        unit_of[jnp.bitwise_xor(server_ref[u], me)] = u


def pack_kernel(server_ref, place_ref, q_ref, k_ref, v_ref, g_ref, *rest):
    out_refs, unit_of = rest[:-1], rest[-1]
    unit_rows = out_refs[0].shape[0]
    find_units(server_ref, unit_of, len(out_refs))
    for k, out_ref in enumerate(out_refs):
        u = unit_of[k]
        rows = pl.ds(pl.multiple_of(u * unit_rows, unit_rows), unit_rows)
        at = 0
        for ref in (q_ref, k_ref, v_ref, g_ref):
            width = ref.shape[1]
            out_ref[:, at : at + width] = ref[rows, :]
            at += width
        place = jnp.full((unit_rows, LANES), place_ref[u], jnp.int32)
        out_ref[:, at : at + LANES] = place.astype(jnp.float32).astype(out_ref.dtype)


def pack(unit_server, unit_place, q, k, v, g):
    units = unit_server.shape[0]
    width = q.shape[1] + k.shape[1] + v.shape[1] + g.shape[1] + LANES
    piece = jax.ShapeDtypeStruct((q.shape[0] // units, width), q.dtype)
    return pl.pallas_call(
        pack_kernel,
        out_shape=[piece] * units,
        in_specs=[SMEM, SMEM, VMEM, VMEM, VMEM, VMEM],
        out_specs=[VMEM] * units,
        scratch_shapes=[pltpu.SMEM((units,), jnp.int32)],
        compiler_params=pltpu.CompilerParams(vmem_limit_bytes=PACK_VMEM),
        name="pack",
    )(unit_server, unit_place, q, k, v, g)


def weight_copies(hbm_refs, vmem_refs, sems, n, r, part_width):
    part = jnp.bitwise_xor(lax.axis_index("mp"), r)
    source = pl.ds(pl.multiple_of(part * part_width, part_width), part_width)
    return [
        pltpu.make_async_copy(hbm.at[source], vmem.at[n], sems.at[n, i])
        for i, (hbm, vmem) in enumerate(zip(hbm_refs, vmem_refs))
    ]


def project(grads, weights, n, store, part_width):
    tile = min(COLUMNS, part_width)
    for at in range(0, part_width, tile):
        total = None
        left = 0
        for weight in weights:
            width = weight.shape[2]
            term = dot(grads[:, left : left + width], weight[n, at : at + tile, :], NT)
            total = term if total is None else total + term
            left += width
        store(at, tile, total.astype(BF16))


def serve_kernel(kv_heads, parts, sizes, length_ref, *refs):
    servers = sum(sizes)
    arrived = refs[:servers]
    hbm_refs = refs[servers : servers + 3]
    grads = refs[servers + 3]
    out_refs = refs[servers + 4 : servers + 4 + len(sizes)]
    qw, kw, vw, bias, queries, masked, probs_low, score_low, sems = refs[servers + 4 + len(sizes) :]
    unit_rows = arrived[0].shape[0]
    rows = servers * unit_rows
    doc_count = length_ref.shape[0]
    part_width = qw.shape[1]
    q_width = qw.shape[2]
    kv_width = kw.shape[2]
    group = q_width // kv_width
    scale = 1.0 / math.sqrt(HEAD)
    score_scale = scale * math.log2(math.e)

    def copies(n):
        return weight_copies(hbm_refs, (qw, kw, vw), sems, n, parts[n], part_width)

    for n in range(len(parts)):
        for copy in copies(n):
            copy.start()

    def load(at, width):
        return jnp.concatenate([ref[:, at : at + width] for ref in arrived], axis=0)

    place = load(2 * (q_width + kv_width), LANES).astype(jnp.float32)
    row = lax.broadcasted_iota(jnp.int32, (rows, LANES), 0).astype(jnp.float32)
    doc = jnp.floor(place * (1.0 / DOC_UNITS))
    position = (place - DOC_UNITS * doc) * unit_rows
    position = position + (row - unit_rows * jnp.floor(row * (1.0 / unit_rows)))
    length = jnp.full((rows, LANES), length_ref[0], jnp.int32).astype(jnp.float32)
    for d in range(1, doc_count):
        length = jnp.where(doc == d, length_ref[d].astype(jnp.float32), length)
    live = position < length
    key_at = jnp.where(live, position, 1e9)[:, :1]
    allowed = key_at <= jnp.transpose(position)[:1, :]
    if doc_count > 1:
        allowed = allowed & (doc[:, :1] == jnp.transpose(doc)[:1, :])
    bias[...] = jnp.where(allowed, 0.0, -1e30)
    tiles = rows // TILE
    for kv in range(kv_heads):
        keys = load(q_width + kv * HEAD, HEAD)
        values = load(q_width + kv_width + kv * HEAD, HEAD)
        for h in range(group):
            head = kv * group + h
            here = slice(h * rows, (h + 1) * rows)
            queries[here, :] = load(head * HEAD, HEAD)
            outer = load(q_width + 2 * kv_width + head * HEAD, HEAD).astype(jnp.float32)
            masked[here, :] = jnp.where(live, outer, 0.0).astype(BF16)
        for t in range(group * tiles):
            at = t * TILE
            within = (t % tiles) * TILE
            scores = dot(keys, queries[at : at + TILE, :], NT) * score_scale
            scores = scores + bias[:, within : within + TILE]
            peak = jnp.max(scores, axis=0, keepdims=True)
            expanded = jnp.exp2(scores - peak)
            probs = expanded * (1.0 / jnp.sum(expanded, axis=0, keepdims=True))
            low = probs.astype(BF16)
            probs_low[:, at : at + TILE] = low
            prob_grad = dot(values, masked[at : at + TILE, :], NT)
            delta = jnp.sum(low.astype(jnp.float32) * prob_grad, axis=0, keepdims=True)
            score_low[:, at : at + TILE] = (probs * (prob_grad - delta)).astype(BF16)
        at = q_width + kv * HEAD
        grads[:, at : at + HEAD] = (dot(score_low[...], queries[...], NN) * scale).astype(BF16)
        at = q_width + kv_width + kv * HEAD
        grads[:, at : at + HEAD] = dot(probs_low[...], masked[...], NN).astype(BF16)
        for h in range(group):
            at = (kv * group + h) * HEAD
            grads[:, at : at + HEAD] = (
                dot(score_low[:, h * rows : (h + 1) * rows], keys, TN) * scale
            ).astype(BF16)

    for n in range(len(parts)):
        for copy in copies(n):
            copy.wait()

        def store(at, tile, value):
            first = 0
            for size, out_ref in zip(sizes, out_refs):
                piece = value[first * unit_rows : (first + size) * unit_rows, :]
                out_ref[n, :, :, at : at + tile] = piece.reshape(size, unit_rows, tile)
                first += size

        project(grads, (qw, kw, vw), n, store, part_width)


def weight_scratch(count, part_width, weights):
    return [pltpu.VMEM((count, part_width, w.shape[1]), BF16) for w in weights] + [
        pltpu.SemaphoreType.DMA((count, len(weights)))
    ]


def serve(doc_length, arrived, weights, parts, sizes, part_width):
    qw, kw, _ = weights
    unit_rows = arrived[0].shape[0]
    rows = unit_rows * len(arrived)
    group = qw.shape[1] // kw.shape[1]
    kv_heads = kw.shape[1] // HEAD
    width = qw.shape[1] + 2 * kw.shape[1]
    *buffers, sems = weight_scratch(len(parts), part_width, weights)
    flops = 2 * rows * width * part_width * len(parts)
    flops += 10 * rows * rows * qw.shape[1]
    return pl.pallas_call(
        functools.partial(serve_kernel, kv_heads, parts, sizes),
        out_shape=[jax.ShapeDtypeStruct((rows, width), BF16)]
        + [
            jax.ShapeDtypeStruct((len(parts), size, unit_rows, part_width), BF16)
            for size in sizes
        ],
        in_specs=[SMEM] + [VMEM] * len(arrived) + [HBM] * 3,
        out_specs=[VMEM] * (1 + len(sizes)),
        scratch_shapes=buffers
        + [
            pltpu.VMEM((rows, rows), jnp.float32),
            pltpu.VMEM((group * rows, HEAD), BF16),
            pltpu.VMEM((group * rows, HEAD), BF16),
            pltpu.VMEM((rows, group * rows), BF16),
            pltpu.VMEM((rows, group * rows), BF16),
            sems,
        ],
        compiler_params=pltpu.CompilerParams(vmem_limit_bytes=SERVE_VMEM),
        cost_estimate=pl.CostEstimate(flops=flops, bytes_accessed=0, transcendentals=0),
        name="serve",
    )(doc_length, *arrived, *weights)


def rest_kernel(parts, grads, qw_hbm, kw_hbm, vw_hbm, out_ref, qw, kw, vw, sems):
    part_width = qw.shape[1]
    _, slots, unit_rows, _ = out_ref.shape

    def copies(n):
        return weight_copies((qw_hbm, kw_hbm, vw_hbm), (qw, kw, vw), sems, n, parts[n], part_width)

    for n in range(len(parts)):
        for copy in copies(n):
            copy.start()
    for n in range(len(parts)):
        for copy in copies(n):
            copy.wait()

        def store(at, tile, value):
            out_ref[n, :, :, at : at + tile] = value.reshape(slots, unit_rows, tile)

        project(grads, (qw, kw, vw), n, store, part_width)


def rest(grads, weights, parts, slots, part_width):
    rows, width = grads.shape
    return pl.pallas_call(
        functools.partial(rest_kernel, parts),
        out_shape=jax.ShapeDtypeStruct((len(parts), slots, rows // slots, part_width), BF16),
        in_specs=[VMEM] + [HBM] * 3,
        out_specs=VMEM,
        scratch_shapes=weight_scratch(len(parts), part_width, weights),
        compiler_params=pltpu.CompilerParams(vmem_limit_bytes=REST_VMEM),
        cost_estimate=pl.CostEstimate(
            flops=2 * rows * width * part_width * len(parts), bytes_accessed=0, transcendentals=0
        ),
        name="rest",
    )(grads, *weights)


def combine_kernel(first, here_ref, there_ref, *out_refs):
    count, size = there_ref.shape[:2]
    for n in range(count):
        for i in range(size):
            total = here_ref[n, first + i].astype(jnp.float32)
            total = total + there_ref[n, i].astype(jnp.float32)
            out_refs[n * size + i][...] = total.astype(BF16)


def combine(here, there, first):
    count, size, unit_rows, width = there.shape
    outs = pl.pallas_call(
        functools.partial(combine_kernel, first),
        out_shape=[jax.ShapeDtypeStruct((unit_rows, width), BF16)] * (count * size),
        in_specs=[VMEM, VMEM],
        out_specs=[VMEM] * (count * size),
        compiler_params=pltpu.CompilerParams(vmem_limit_bytes=SERVE_VMEM),
        name="combine",
    )(here, there)
    return [outs[n * size : (n + 1) * size] for n in range(count)]


def sum_kernel(server_ref, *refs):
    out_hbm, total, unit_of, sems = refs[-4:]
    units, unit_rows, _ = total.shape
    near, far = refs[:units], refs[units : 2 * units]
    find_units(server_ref, unit_of, units)

    def out_copy(k):
        at = pl.multiple_of(unit_of[k] * unit_rows, unit_rows)
        return pltpu.make_async_copy(total.at[k], out_hbm.at[pl.ds(at, unit_rows)], sems.at[k])

    for k in range(units):
        total[k] = near[k][...].astype(jnp.float32) + far[k][...].astype(jnp.float32)
        out_copy(k).start()
    for k in range(units):
        out_copy(k).wait()


def final_sum(unit_server, near, far):
    units = len(near)
    unit_rows, width = near[0].shape
    return pl.pallas_call(
        sum_kernel,
        out_shape=jax.ShapeDtypeStruct((units * unit_rows, width), jnp.float32),
        in_specs=[SMEM] + [VMEM] * (2 * units),
        out_specs=pl.BlockSpec(memory_space=pl.ANY),
        scratch_shapes=[
            pltpu.VMEM((units, unit_rows, width), jnp.float32),
            pltpu.SMEM((units,), jnp.int32),
            pltpu.SemaphoreType.DMA((units,)),
        ],
        compiler_params=pltpu.CompilerParams(vmem_limit_bytes=SUM_VMEM),
        name="final_sum",
    )(unit_server, *near, *far)


def arrival_order(servers):
    return sorted(range(1, servers), key=lambda k: (-(k >> 1).bit_count(), k & 1, k))


def home_groups(servers):
    order = list(range(servers - 1, -1, -1))
    cuts = [0] + [servers * cut // 8 for cut in CUTS] + [servers]
    return [order[a:b] for a, b in zip(cuts, cuts[1:])]


def local(
    saved_query,
    saved_key,
    saved_value,
    grad_output,
    unit_server,
    unit_place,
    doc_length,
    query_weight,
    key_weight,
    value_weight,
):
    servers = lax.axis_size("dp")
    planes = lax.axis_size("mp")
    if servers & (servers - 1) or planes & (planes - 1) or planes < 4 or servers < 2:
        raise ValueError("mesh size")
    part_width = query_weight.shape[0] // planes
    weights = (query_weight, key_weight, value_weight)

    def dp_swap(value, k):
        return lax.ppermute(value, "dp", [(i, i ^ k) for i in range(servers)])

    def mp_swap(value, bit):
        return lax.ppermute(value, "mp", [(i, i ^ bit) for i in range(planes)])

    def both_swap(value, k, bit):
        pairs = [
            (d * planes + z, (d ^ k) * planes + (z ^ bit))
            for d in range(servers)
            for z in range(planes)
        ]
        return lax.ppermute(value, ("dp", "mp"), pairs)

    pieces = pack(unit_server, unit_place, saved_query, saved_key, saved_value, grad_output)
    arrived = [pieces[0]] + [None] * (servers - 1)
    for k in arrival_order(servers):
        arrived[k] = dp_swap(pieces[k], k)
    groups = home_groups(servers)
    sizes = tuple(len(g) for g in groups)
    odd = tuple(range(1, planes, 2))
    even = tuple(range(0, planes, 2))
    grads, *sent = serve(
        doc_length, [arrived[k] for group in groups for k in group], weights, odd, sizes, part_width
    )
    crossed = []
    for value in sent:
        crossed.append(mp_swap(value, 1))
    kept = rest(grads, weights, even, servers, part_width)
    near = [None] * servers
    far = [None] * servers
    first = 0
    for group, there in zip(groups, crossed):
        outs = None
        if planes > 4:
            total = kept[:, first : first + len(group)] + there
            bit = 2
            while bit < planes // 2:
                total = total[0::2] + mp_swap(total[1::2], bit)
                bit *= 2
            outs = [[total[n, m] for m in range(len(group))] for n in range(2)]
        else:
            outs = combine(kept, there, first)
        first += len(group)
        for m, k in enumerate(group):
            far[k] = both_swap(outs[1][m], k, planes // 2)
            near[k] = dp_swap(outs[0][m], k) if k else outs[0][m]
    return final_sum(unit_server, near, far)


def solution(mesh):
    placed = (
        P("dp", "mp"),
        P("dp", "mp"),
        P("dp", "mp"),
        P("dp", "mp"),
        P("dp"),
        P("dp"),
        P("dp"),
        P(None, "mp"),
        P(None, "mp"),
        P(None, "mp"),
    )
    return jax.shard_map(
        local, mesh=mesh, in_specs=placed, out_specs=P("dp", "mp"), check_vma=False
    )
```

```python
import functools
import math

import jax
import jax.numpy as jnp
from jax import lax
from jax.experimental import pallas as pl
from jax.experimental.pallas import tpu as pltpu
from jax.sharding import PartitionSpec as P


HEAD = 128
DOC_UNITS = 8
LANES = 128
TILE = 256
CUTS = (1, 3, 5, 7)
COLUMNS = 256
PACK_VMEM = 60 << 20
SERVE_VMEM = 50 << 20
REST_VMEM = 52 << 20
SUM_VMEM = 12 << 20
SPLIT = 2


NN = (((1,), (0,)), ((), ()))
NT = (((1,), (1,)), ((), ()))
TN = (((0,), (0,)), ((), ()))

SMEM = pl.BlockSpec(memory_space=pltpu.SMEM)
VMEM = pl.BlockSpec(memory_space=pltpu.VMEM)
HBM = pl.BlockSpec(memory_space=pltpu.HBM)
BF16 = jnp.bfloat16


def dot(a, b, numbers):
    return lax.dot_general(a, b, numbers, preferred_element_type=jnp.float32)


def find_units(server_ref, unit_of, servers):
    me = lax.axis_index("dp")
    for u in range(servers):
        unit_of[jnp.bitwise_xor(server_ref[u], me)] = u


def pack_kernel(server_ref, place_ref, q_ref, k_ref, v_ref, g_ref, *rest):
    out_refs, unit_of = rest[:-1], rest[-1]
    unit_rows = out_refs[0].shape[0]
    find_units(server_ref, unit_of, len(out_refs))
    for k, out_ref in enumerate(out_refs):
        u = unit_of[k]
        rows = pl.ds(pl.multiple_of(u * unit_rows, unit_rows), unit_rows)
        at = 0
        for ref in (q_ref, k_ref, v_ref, g_ref):
            width = ref.shape[1]
            out_ref[:, at : at + width] = ref[rows, :]
            at += width
        place = jnp.full((unit_rows, LANES), place_ref[u], jnp.int32)
        out_ref[:, at : at + LANES] = place.astype(jnp.float32).astype(out_ref.dtype)


def pack(unit_server, unit_place, q, k, v, g):
    units = unit_server.shape[0]
    width = q.shape[1] + k.shape[1] + v.shape[1] + g.shape[1] + LANES
    piece = jax.ShapeDtypeStruct((q.shape[0] // units, width), q.dtype)
    return pl.pallas_call(
        pack_kernel,
        out_shape=[piece] * units,
        in_specs=[SMEM, SMEM, VMEM, VMEM, VMEM, VMEM],
        out_specs=[VMEM] * units,
        scratch_shapes=[pltpu.SMEM((units,), jnp.int32)],
        compiler_params=pltpu.CompilerParams(vmem_limit_bytes=PACK_VMEM),
        name="pack",
    )(unit_server, unit_place, q, k, v, g)


def keep_kernel(in_ref, out_ref):
    out_ref[...] = in_ref[...]


def keep(piece):
    return pl.pallas_call(
        keep_kernel,
        out_shape=jax.ShapeDtypeStruct(piece.shape, piece.dtype),
        in_specs=[VMEM],
        out_specs=VMEM,
        compiler_params=pltpu.CompilerParams(vmem_limit_bytes=SERVE_VMEM),
        name="keep",
    )(piece)


def weight_copies(hbm_refs, vmem_refs, sems, n, r, part_width):
    part = jnp.bitwise_xor(lax.axis_index("mp"), r)
    source = pl.ds(pl.multiple_of(part * part_width, part_width), part_width)
    return [
        pltpu.make_async_copy(hbm.at[source], vmem.at[n], sems.at[n, i])
        for i, (hbm, vmem) in enumerate(zip(hbm_refs, vmem_refs))
    ]


def project(grads, weights, n, store, part_width):
    tile = min(COLUMNS, part_width)
    for at in range(0, part_width, tile):
        total = None
        left = 0
        for weight in weights:
            width = weight.shape[2]
            term = dot(grads[:, left : left + width], weight[n, at : at + tile, :], NT)
            total = term if total is None else total + term
            left += width
        store(at, tile, total.astype(BF16))


def serve_kernel(kv_heads, parts, sizes, length_ref, *refs):
    servers = sum(sizes)
    arrived = refs[:servers]
    hbm_refs = refs[servers : servers + 3]
    grads = refs[servers + 3]
    out_refs = refs[servers + 4 : servers + 4 + len(sizes)]
    qw, kw, vw, bias, queries, masked, probs_low, score_low, sems = refs[servers + 4 + len(sizes) :]
    unit_rows = arrived[0].shape[0]
    rows = servers * unit_rows
    doc_count = length_ref.shape[0]
    part_width = qw.shape[1]
    q_width = qw.shape[2]
    kv_width = kw.shape[2]
    group = q_width // kv_width
    scale = 1.0 / math.sqrt(HEAD)
    score_scale = scale * math.log2(math.e)

    def copies(n):
        return weight_copies(hbm_refs, (qw, kw, vw), sems, n, parts[n], part_width)

    for n in range(len(parts)):
        for copy in copies(n):
            copy.start()

    def load(at, width):
        return jnp.concatenate([ref[:, at : at + width] for ref in arrived], axis=0)

    place = load(2 * (q_width + kv_width), LANES).astype(jnp.float32)
    row = lax.broadcasted_iota(jnp.int32, (rows, LANES), 0).astype(jnp.float32)
    doc = jnp.floor(place * (1.0 / DOC_UNITS))
    position = (place - DOC_UNITS * doc) * unit_rows
    position = position + (row - unit_rows * jnp.floor(row * (1.0 / unit_rows)))
    length = jnp.full((rows, LANES), length_ref[0], jnp.int32).astype(jnp.float32)
    for d in range(1, doc_count):
        length = jnp.where(doc == d, length_ref[d].astype(jnp.float32), length)
    live = position < length
    key_at = jnp.where(live, position, 1e9)[:, :1]
    allowed = key_at <= jnp.transpose(position)[:1, :]
    if doc_count > 1:
        allowed = allowed & (doc[:, :1] == jnp.transpose(doc)[:1, :])
    bias[...] = jnp.where(allowed, 0.0, -1e30)
    tiles = rows // TILE
    for kv in range(kv_heads):
        keys = load(q_width + kv * HEAD, HEAD)
        values = load(q_width + kv_width + kv * HEAD, HEAD)
        for h in range(group):
            head = kv * group + h
            here = slice(h * rows, (h + 1) * rows)
            queries[here, :] = load(head * HEAD, HEAD)
            outer = load(q_width + 2 * kv_width + head * HEAD, HEAD).astype(jnp.float32)
            masked[here, :] = jnp.where(live, outer, 0.0).astype(BF16)
        for t in range(group * tiles):
            at = t * TILE
            within = (t % tiles) * TILE
            scores = dot(keys, queries[at : at + TILE, :], NT) * score_scale
            scores = scores + bias[:, within : within + TILE]
            peak = jnp.max(scores, axis=0, keepdims=True)
            expanded = jnp.exp2(scores - peak)
            probs = expanded * (1.0 / jnp.sum(expanded, axis=0, keepdims=True))
            low = probs.astype(BF16)
            probs_low[:, at : at + TILE] = low
            prob_grad = dot(values, masked[at : at + TILE, :], NT)
            delta = jnp.sum(low.astype(jnp.float32) * prob_grad, axis=0, keepdims=True)
            score_low[:, at : at + TILE] = (probs * (prob_grad - delta)).astype(BF16)
        at = q_width + kv * HEAD
        grads[:, at : at + HEAD] = (dot(score_low[...], queries[...], NN) * scale).astype(BF16)
        at = q_width + kv_width + kv * HEAD
        grads[:, at : at + HEAD] = dot(probs_low[...], masked[...], NN).astype(BF16)
        for h in range(group):
            at = (kv * group + h) * HEAD
            grads[:, at : at + HEAD] = (
                dot(score_low[:, h * rows : (h + 1) * rows], keys, TN) * scale
            ).astype(BF16)

    for n in range(len(parts)):
        for copy in copies(n):
            copy.wait()

        def store(at, tile, value):
            first = 0
            for size, out_ref in zip(sizes, out_refs):
                piece = value[first * unit_rows : (first + size) * unit_rows, :]
                out_ref[n, :, :, at : at + tile] = piece.reshape(size, unit_rows, tile)
                first += size

        project(grads, (qw, kw, vw), n, store, part_width)


def weight_scratch(count, part_width, weights):
    return [pltpu.VMEM((count, part_width, w.shape[1]), BF16) for w in weights] + [
        pltpu.SemaphoreType.DMA((count, len(weights)))
    ]


def serve(doc_length, arrived, weights, parts, sizes, part_width):
    qw, kw, _ = weights
    unit_rows = arrived[0].shape[0]
    rows = unit_rows * len(arrived)
    group = qw.shape[1] // kw.shape[1]
    kv_heads = kw.shape[1] // HEAD
    width = qw.shape[1] + 2 * kw.shape[1]
    *buffers, sems = weight_scratch(len(parts), part_width, weights)
    flops = 2 * rows * width * part_width * len(parts)
    flops += 10 * rows * rows * qw.shape[1]
    return pl.pallas_call(
        functools.partial(serve_kernel, kv_heads, parts, sizes),
        out_shape=[jax.ShapeDtypeStruct((rows, width), BF16)]
        + [
            jax.ShapeDtypeStruct((len(parts), size, unit_rows, part_width), BF16)
            for size in sizes
        ],
        in_specs=[SMEM] + [VMEM] * len(arrived) + [HBM] * 3,
        out_specs=[VMEM] * (1 + len(sizes)),
        scratch_shapes=buffers
        + [
            pltpu.VMEM((rows, rows), jnp.float32),
            pltpu.VMEM((group * rows, HEAD), BF16),
            pltpu.VMEM((group * rows, HEAD), BF16),
            pltpu.VMEM((rows, group * rows), BF16),
            pltpu.VMEM((rows, group * rows), BF16),
            sems,
        ],
        compiler_params=pltpu.CompilerParams(vmem_limit_bytes=SERVE_VMEM),
        cost_estimate=pl.CostEstimate(flops=flops, bytes_accessed=0, transcendentals=0),
        name="serve",
    )(doc_length, *arrived, *weights)


def rest_kernel(parts, grads, qw_hbm, kw_hbm, vw_hbm, out_ref, qw, kw, vw, sems):
    part_width = qw.shape[1]
    _, slots, unit_rows, _ = out_ref.shape

    def copies(n):
        return weight_copies((qw_hbm, kw_hbm, vw_hbm), (qw, kw, vw), sems, n, parts[n], part_width)

    for n in range(len(parts)):
        for copy in copies(n):
            copy.start()
    for n in range(len(parts)):
        for copy in copies(n):
            copy.wait()

        def store(at, tile, value):
            out_ref[n, :, :, at : at + tile] = value.reshape(slots, unit_rows, tile)

        project(grads, (qw, kw, vw), n, store, part_width)


def rest(grads, weights, parts, slots, part_width):
    rows, width = grads.shape
    return pl.pallas_call(
        functools.partial(rest_kernel, parts),
        out_shape=jax.ShapeDtypeStruct((len(parts), slots, rows // slots, part_width), BF16),
        in_specs=[VMEM] + [HBM] * 3,
        out_specs=VMEM,
        scratch_shapes=weight_scratch(len(parts), part_width, weights),
        compiler_params=pltpu.CompilerParams(vmem_limit_bytes=REST_VMEM),
        cost_estimate=pl.CostEstimate(
            flops=2 * rows * width * part_width * len(parts), bytes_accessed=0, transcendentals=0
        ),
        name="rest",
    )(grads, *weights)


def combine_kernel(first, here_ref, there_ref, *out_refs):
    count, size = there_ref.shape[:2]
    for n in range(count):
        for i in range(size):
            total = here_ref[n, first + i].astype(jnp.float32)
            total = total + there_ref[n, i].astype(jnp.float32)
            out_refs[n * size + i][...] = total.astype(BF16)


def combine(here, there, first):
    count, size, unit_rows, width = there.shape
    outs = pl.pallas_call(
        functools.partial(combine_kernel, first),
        out_shape=[jax.ShapeDtypeStruct((unit_rows, width), BF16)] * (count * size),
        in_specs=[VMEM, VMEM],
        out_specs=[VMEM] * (count * size),
        compiler_params=pltpu.CompilerParams(vmem_limit_bytes=SERVE_VMEM),
        name="combine",
    )(here, there)
    return [outs[n * size : (n + 1) * size] for n in range(count)]


def sum_kernel(slots, server_ref, *refs):
    out_hbm, total, unit_of, sems = refs[-4:]
    servers = unit_of.shape[0]
    count, unit_rows, _ = total.shape
    find_units(server_ref, unit_of, servers)

    def out_copy(i):
        at = pl.multiple_of(unit_of[slots[i]] * unit_rows, unit_rows)
        return pltpu.make_async_copy(total.at[i], out_hbm.at[pl.ds(at, unit_rows)], sems.at[i])

    for i in range(count):
        total[i] = refs[i][...].astype(jnp.float32) + refs[count + i][...].astype(jnp.float32)
        out_copy(i).start()
    for i in range(count):
        out_copy(i).wait()


def place_sums(unit_server, slots, near, far, out):
    servers = unit_server.shape[0]
    unit_rows, width = near[0].shape
    count = len(slots)
    hbm = pl.BlockSpec(memory_space=pl.ANY)
    return pl.pallas_call(
        functools.partial(sum_kernel, tuple(slots)),
        out_shape=jax.ShapeDtypeStruct((servers * unit_rows, width), jnp.float32),
        in_specs=[SMEM] + [VMEM] * (2 * count) + [hbm] * len(out),
        out_specs=hbm,
        input_output_aliases={1 + 2 * count: 0} if out else {},
        scratch_shapes=[
            pltpu.VMEM((count, unit_rows, width), jnp.float32),
            pltpu.SMEM((servers,), jnp.int32),
            pltpu.SemaphoreType.DMA((count,)),
        ],
        compiler_params=pltpu.CompilerParams(vmem_limit_bytes=SUM_VMEM),
        name="place_sums",
    )(unit_server, *near, *far, *out)


def arrival_order(servers):
    return sorted(range(1, servers), key=lambda k: (k == 1, k & 1, -(k >> 1).bit_count(), k))


def home_groups(servers):
    order = list(range(servers - 1, -1, -1))
    cuts = [0] + [servers * cut // 8 for cut in CUTS] + [servers]
    return [order[a:b] for a, b in zip(cuts, cuts[1:])]


def local(
    saved_query,
    saved_key,
    saved_value,
    grad_output,
    unit_server,
    unit_place,
    doc_length,
    query_weight,
    key_weight,
    value_weight,
):
    servers = lax.axis_size("dp")
    planes = lax.axis_size("mp")
    if servers & (servers - 1) or planes & (planes - 1) or planes < 4 or servers < 2:
        raise ValueError("mesh size")
    part_width = query_weight.shape[0] // planes
    weights = (query_weight, key_weight, value_weight)

    def dp_swap(value, k):
        return lax.ppermute(value, "dp", [(i, i ^ k) for i in range(servers)])

    def mp_swap(value, bit):
        return lax.ppermute(value, "mp", [(i, i ^ bit) for i in range(planes)])

    def both_swap(value, k, bit):
        pairs = [
            (d * planes + z, (d ^ k) * planes + (z ^ bit))
            for d in range(servers)
            for z in range(planes)
        ]
        return lax.ppermute(value, ("dp", "mp"), pairs)

    pieces = pack(unit_server, unit_place, saved_query, saved_key, saved_value, grad_output)
    arrived = [keep(pieces[0])] + [None] * (servers - 1)
    for k in arrival_order(servers):
        arrived[k] = dp_swap(pieces[k], k)
    groups = home_groups(servers)
    sizes = tuple(len(g) for g in groups)
    odd = tuple(range(1, planes, 2))
    even = tuple(range(0, planes, 2))
    grads, *sent = serve(
        doc_length, [arrived[k] for group in groups for k in group], weights, odd, sizes, part_width
    )
    crossed = []
    for value in sent:
        crossed.append(mp_swap(value, 1))
    kept = rest(grads, weights, even, servers, part_width)
    near = [None] * servers
    far = [None] * servers
    first = 0
    for group, there in zip(groups, crossed):
        outs = None
        if planes > 4:
            total = kept[:, first : first + len(group)] + there
            bit = 2
            while bit < planes // 2:
                total = total[0::2] + mp_swap(total[1::2], bit)
                bit *= 2
            outs = [[total[n, m] for m in range(len(group))] for n in range(2)]
        else:
            outs = combine(kept, there, first)
        first += len(group)
        for m, k in enumerate(group):
            far[k] = both_swap(outs[1][m], k, planes // 2)
            near[k] = dp_swap(outs[0][m], k) if k else outs[0][m]
    out = []
    early = len(groups) - SPLIT
    for part in (groups[:early], groups[early:]):
        slots = [k for group in part for k in group]
        out = [
            place_sums(unit_server, slots, [near[k] for k in slots], [far[k] for k in slots], out)
        ]
    return out[0]


def solution(mesh):
    placed = (
        P("dp", "mp"),
        P("dp", "mp"),
        P("dp", "mp"),
        P("dp", "mp"),
        P("dp"),
        P("dp"),
        P("dp"),
        P(None, "mp"),
        P(None, "mp"),
        P(None, "mp"),
    )
    return jax.shard_map(
        local, mesh=mesh, in_specs=placed, out_specs=P("dp", "mp"), check_vma=False
    )
```
